32 devices in a mesh: slab: 16 (over z, x, core), layer: 2 (over y).
Axes of the slice: x: 2, y: 2, z: 4, core: 2. Of those that a mesh axis runs over, the one named last changes fastest.
Arguments:
- nodal_field: float32 [2, 1024, 4, 4, 512], P('layer', 'slab'), may hold values from -6 to 6
- metric: float32 [2, 1024, 4, 4, 3, 512], P('layer', 'slab'), may hold values from 0.25 to 2
- slab_ids: int32 [1024], replicated, may hold values from 0 to 1023, as said below
- face_map: int32 [1024, 1024], P('slab'), may hold values from 0 to 1023, as said below
Outputs:
- assembled: float32 [2, 1024, 4, 4, 512], P('layer', 'slab')
The draws below stay inside these ranges and needn't reach their ends.
Inputs may be any that keep to these rules, and one draw needn't show every extreme that they name: slab_ids is a permutation of 0 to 1023; positions p of one device are those with p // 64 equal to its index along slab, and for one rotation R every device holds exactly the slabs g with (g + R) mod 16 equal to its index, in any order of its positions, so slab (g + 1) mod 1024 always sits on the next device along slab, cyclically. Each row of face_map is a permutation of 0 to 1023: either the identity, or the map that reverses y, sending (ez, ey, c, b) to (ez, 3 - ey, c, 7 - b); z order is never changed.
All inputs are finite; a program needn't handle non-finite values.
Results may differ from the reference program's by a relative error of at most 0.00005.
Values sent between devices are 32-bit elements; how exact they have to be, the bound alone decides.
A program may use at most 192 MiB of HBM per device.

```python
import math
import jax
import jax.numpy as jnp
import numpy as np
from jax import lax

P_SIZE = 8
PTS = 512
EY = 4
EZ = 4
SLAB_DEV = 64
FACE = 1024
SLABS = 1024
LAYERS = 2
N_SLAB = 16


def permute_slots(sub_key):
    return jax.random.permutation(sub_key, SLAB_DEV)


def draw_slab_ids(key, part):
    rotate_key = jax.random.fold_in(key, 11)
    order_key = jax.random.fold_in(key, 12)
    rotation = jax.random.randint(rotate_key, (), 0, N_SLAB)
    key_list = jax.random.split(order_key, N_SLAB)
    slot_orders = jax.vmap(permute_slots)(key_list).astype(jnp.int32)
    residues = (jnp.arange(N_SLAB, dtype=jnp.int32) - rotation + N_SLAB) % N_SLAB
    return (slot_orders * N_SLAB + residues[:, None]).reshape(SLABS).astype(jnp.int32)


def draw_face_map(key, part):
    flip_key = jax.random.fold_in(key, 21)
    flip_bits = jax.random.randint(flip_key, (SLABS, 1), 0, 2)
    point_index = jnp.arange(FACE, dtype=jnp.int32)
    column = point_index % P_SIZE
    element_col = point_index // (P_SIZE * P_SIZE) % EY
    reversed_index = point_index + (P_SIZE - 1 - 2 * column) + (EY - 1 - 2 * element_col) * P_SIZE * P_SIZE
    return jnp.where(flip_bits == 1, reversed_index[None, :], point_index[None, :]).astype(jnp.int32)


def steps_of(rng, dims, shards, low, high):
    loudness, own = 1.0, jax.random.fold_in(rng, 6)
    for position, parts in shards:
        steps = jnp.exp(jax.random.uniform(jax.random.fold_in(own, position), (parts,), jnp.float32, low / len(shards), high / len(shards)))
        loudness = loudness * jnp.repeat(steps, dims[position] // parts).reshape([-1 if axis == position else 1 for axis in range(len(dims))])
    return loudness


def noise(key, shape, spread, limit, cuts=(), kind=jnp.bfloat16):
    drawn = spread * jax.random.normal(key, shape, jnp.float32)
    if cuts:
        drawn = drawn * steps_of(key, shape, cuts, -0.22, 0.18)
    return jnp.clip(drawn, -limit, limit).astype(kind)


def setup_inputs(seed: int = 0) -> dict:
    arg_keys = jax.random.split(jax.random.key(seed), 5)
    nodal_field = noise(arg_keys[0], (LAYERS, SLABS, EZ, EY, PTS), 1.0, 6.0, ((0, 2), (1, 16)), jnp.float32)
    metric = jnp.clip(jnp.exp(math.log(2.0) - 2.0794415 * jax.random.uniform(arg_keys[1], (LAYERS, SLABS, EZ, EY, 3, PTS), jnp.float32) ** steps_of(arg_keys[1], (LAYERS, SLABS, EZ, EY, 3, PTS), ((0, 2), (1, 16)), -0.2, 0.2)), 0.25, 2.0)
    slab_ids = draw_slab_ids(jax.random.fold_in(arg_keys[4], 71), 0)
    face_map = draw_face_map(jax.random.fold_in(arg_keys[4], 71), 0)
    return dict(nodal_field=nodal_field, metric=metric, slab_ids=slab_ids, face_map=face_map)


def legendre_pair(gll_nodes, degree):
    lower_poly = gll_nodes * 0.0 + 1.0
    upper_poly = gll_nodes.copy()
    for poly_order in range(2, degree + 1):
        lower_poly, upper_poly = upper_poly, ((2 * poly_order - 1) * gll_nodes * upper_poly - (poly_order - 1) * lower_poly) / poly_order
    return lower_poly, upper_poly


def gll_tables():
    degree = P_SIZE - 1
    gll_nodes = -np.cos(np.pi * np.arange(P_SIZE) / degree)
    for newton_sweep in range(100):
        lower_poly, upper_poly = legendre_pair(gll_nodes, degree)
        gll_nodes = gll_nodes - (gll_nodes * upper_poly - lower_poly) / ((degree + 1) * upper_poly)
    lower_poly, upper_poly = legendre_pair(gll_nodes, degree)
    quad_weights = 2.0 / (degree * (degree + 1) * upper_poly * upper_poly)
    identity = np.eye(P_SIZE)
    differ = gll_nodes[:, None] - gll_nodes[None, :] + identity
    derivative = upper_poly[:, None] / (upper_poly[None, :] * differ)
    derivative = derivative * (1.0 - identity)
    derivative[0, 0] = -degree * (degree + 1) / 4.0
    derivative[degree, degree] = degree * (degree + 1) / 4.0
    weight_cube = quad_weights[:, None, None] * quad_weights[None, :, None] * quad_weights[None, None, :]
    return jnp.asarray(derivative, jnp.float32), jnp.asarray(weight_cube, jnp.float32)


def local_apply(values, factors, derivative, weight_cube):
    highest = lax.Precision.HIGHEST
    grad_x = jnp.einsum("ai,...cbi->...cba", derivative, values, precision=highest)
    grad_y = jnp.einsum("bi,...cia->...cba", derivative, values, precision=highest)
    grad_z = jnp.einsum("ci,...iba->...cba", derivative, values, precision=highest)
    flux_x = weight_cube * factors[..., 0, :, :, :] * grad_x
    flux_y = weight_cube * factors[..., 1, :, :, :] * grad_y
    flux_z = weight_cube * factors[..., 2, :, :, :] * grad_z
    result = jnp.einsum("ia,...cbi->...cba", derivative, flux_x, precision=highest)
    result = result + jnp.einsum("ib,...cia->...cba", derivative, flux_y, precision=highest)
    result = result + jnp.einsum("ic,...iba->...cba", derivative, flux_z, precision=highest)
    return result


def assemble_slab(values):
    shared = values[..., :, :-1, :, P_SIZE - 1, :] + values[..., :, 1:, :, 0, :]
    values = values.at[..., :, :-1, :, P_SIZE - 1, :].set(shared)
    values = values.at[..., :, 1:, :, 0, :].set(shared)
    shared = values[..., :-1, :, P_SIZE - 1, :, :] + values[..., 1:, :, 0, :, :]
    values = values.at[..., :-1, :, P_SIZE - 1, :, :].set(shared)
    values = values.at[..., 1:, :, 0, :, :].set(shared)
    return values


def face_of(local_out, column):
    return local_out[..., column].reshape(local_out.shape[:-5] + (FACE,))


def put_face(local_out, face_values, column):
    return local_out.at[..., column].set(face_values.reshape(local_out.shape[:-1]))


def reference(nodal_field, metric, slab_ids, face_map):
    derivative, weight_cube = gll_tables()
    values = nodal_field.reshape(LAYERS * N_SLAB, SLAB_DEV, EZ, EY, P_SIZE, P_SIZE, P_SIZE)
    factors = metric.reshape(LAYERS * N_SLAB, SLAB_DEV, EZ, EY, 3, P_SIZE, P_SIZE, P_SIZE)

    def slab_block(pair_in):
        return assemble_slab(local_apply(pair_in[0], pair_in[1], derivative, weight_cube))

    local_out = lax.map(slab_block, (values, factors)).reshape(LAYERS, SLABS, EZ, EY, P_SIZE, P_SIZE, P_SIZE)
    slab_iota = jnp.arange(SLABS, dtype=jnp.int32)
    inverse = jnp.zeros((SLABS,), jnp.int32).at[slab_ids].set(slab_iota)
    next_pos = inverse[(slab_ids + 1) % SLABS]
    prev_pos = inverse[(slab_ids + SLABS - 1) % SLABS]
    right_face = face_of(local_out, P_SIZE - 1)
    left_face = face_of(local_out, 0)
    reoriented = jnp.zeros_like(right_face).at[:, slab_iota[:, None], face_map].set(right_face)
    left_sum = left_face + reoriented[:, prev_pos]
    right_sum = right_face + jnp.take_along_axis(left_face[:, next_pos], face_map[None, :, :], axis=2)
    local_out = put_face(local_out, left_sum, 0)
    local_out = put_face(local_out, right_sum, P_SIZE - 1)
    top_face = local_out[:, :, EZ - 1, :, P_SIZE - 1, :, :]
    bottom_face = local_out[:, :, 0, :, 0, :, :]
    top_sum = top_face + jnp.roll(bottom_face, -1, axis=0)
    bottom_sum = bottom_face + jnp.roll(top_face, 1, axis=0)
    local_out = local_out.at[:, :, 0, :, 0, :, :].set(bottom_sum)
    local_out = local_out.at[:, :, EZ - 1, :, P_SIZE - 1, :, :].set(top_sum)
    return local_out.reshape(LAYERS, SLABS, EZ, EY, PTS)
```

```python
import functools

import jax
import jax.numpy as jnp
import numpy as np
from jax import lax
from jax.experimental import pallas as pl
from jax.experimental.pallas import tpu as pltpu
from jax.sharding import PartitionSpec as P

P_SIZE = 8
PTS = 512
EY = 4
EZ = 4
SUB = 8
LANES = 128
SB = 8
DEPTH = 3
GROUP = 16


def legendre_pair(nodes, degree):
    lower = nodes * 0.0 + 1.0
    upper = nodes.copy()
    for order in range(2, degree + 1):
        lower, upper = upper, ((2 * order - 1) * nodes * upper - (order - 1) * lower) / order
    return lower, upper


def gll_tables():
    degree = P_SIZE - 1
    nodes = -np.cos(np.pi * np.arange(P_SIZE) / degree)
    for _ in range(100):
        lower, upper = legendre_pair(nodes, degree)
        nodes = nodes - (nodes * upper - lower) / ((degree + 1) * upper)
    lower, upper = legendre_pair(nodes, degree)
    rho = 2.0 / (degree * (degree + 1) * upper * upper)
    eye = np.eye(P_SIZE)
    differ = nodes[:, None] - nodes[None, :] + eye
    der = upper[:, None] / (upper[None, :] * differ) * (1.0 - eye)
    der[0, 0] = -degree * (degree + 1) / 4.0
    der[degree, degree] = degree * (degree + 1) / 4.0
    return der, rho


def two_parts(table):
    high = np.asarray(table, np.float32).astype(jnp.bfloat16)
    low = (table - high.astype(np.float64)).astype(jnp.bfloat16)
    return high, low


def tables():
    der, rho = gll_tables()
    eye8, eye2 = np.eye(8), np.eye(2)
    plane = np.tile(np.kron(rho, rho), 2)
    fwd = np.concatenate(
        [np.kron(np.eye(16), der.T) * plane, np.kron(eye2, np.kron(der.T, eye8)) * plane], 1
    )
    high, low = two_parts(fwd)
    fwd_op = np.concatenate([high, high, low], 0)
    bwd = np.concatenate([np.kron(np.eye(16), der), np.kron(eye2, np.kron(der, eye8))], 0)
    high, low = two_parts(bwd)
    half = np.concatenate([high, low], 1)
    bwd_op = np.concatenate([half, half], 0)
    l2 = (np.arange(SUB) // EY)[:, None]
    h = (np.arange(LANES) // 64)[None, :]
    cube_plane = plane[None, :]
    zf = np.zeros((2, 2, 2, 2, SUB, LANES))
    zb = np.zeros((2, 2, 2, 2, SUB, LANES))
    rc = np.zeros((2, SUB, LANES))
    for lo in range(2):
        c_out = 2 * (2 * lo + l2) + h
        rc[lo] = rho[c_out]
        for li in range(2):
            for s in range(2):
                for l in range(2):
                    c_in = 2 * (2 * li + (l2 ^ s)) + (h ^ l)
                    zf[lo, l, li, s] = np.roll(der[c_out, c_in] * rho[c_out] * cube_plane, 64 * l, 1)
                    zb[lo, l, li, s] = np.roll(der[c_in, c_out], 64 * l, 1)
    consts = np.concatenate([zf.reshape(-1, SUB, LANES), zb.reshape(-1, SUB, LANES), rc], 0)
    return fwd_op, bwd_op, consts.astype(np.float32)


def roll_sub(x, by):
    return pltpu.roll(x, by % SUB, axis=x.ndim - 2)


def roll_lane(x, by):
    return pltpu.roll(x, by % LANES, axis=x.ndim - 1)


def split(x):
    high = x.astype(jnp.bfloat16)
    return high, (x - high.astype(jnp.float32)).astype(jnp.bfloat16)


def iotas():
    sub = lax.broadcasted_iota(jnp.int32, (SUB, LANES), 0)
    lane = lax.broadcasted_iota(jnp.int32, (SUB, LANES), 1)
    return sub, lane


def lane_gather(x, index):
    return jnp.take_along_axis(x, index, axis=1, mode="promise_in_bounds")


def flip(x, sub, lane):
    y = lane_gather(x, lane ^ 7)
    y = jnp.where(sub % 2 == 0, roll_sub(y, -1), roll_sub(y, 1))
    return jnp.where(sub % EY < 2, roll_sub(y, -2), roll_sub(y, 2))


def sum_of(parts):
    return (parts[0] + parts[1]) + (parts[2] + parts[3])


def apply_z(pair, consts, base):
    terms = []
    for v in pair:
        terms += [v, roll_sub(v, 4)]
    out = []
    for lo in range(2):
        near, far = (
            sum_of([consts[base + 8 * lo + 4 * half + t] * terms[t] for t in range(4)])
            for half in range(2)
        )
        out.append(near + roll_lane(far, 64))
    return out


def local_work(sb, u, m, fwd, bwd, consts, put_w):
    rows = sb * 64
    high, low = split(u)
    g = jnp.dot(jnp.concatenate([high, low, high], 1), fwd, preferred_element_type=jnp.float32)
    m = m.reshape(sb * EZ, 3, 16, LANES)
    gx = g[:, :LANES].reshape(sb * EZ, 16, LANES)
    gy = g[:, LANES:].reshape(sb * EZ, 16, LANES)
    fx = (gx * m[:, 0]).reshape(rows, LANES)
    fy = (gy * m[:, 1]).reshape(rows, LANES)
    xh, xl = split(fx)
    yh, yl = split(fy)
    r = jnp.dot(jnp.concatenate([xh, yh, xl, yl], 1), bwd, preferred_element_type=jnp.float32)
    r = (r[:, :LANES] + r[:, LANES:]).reshape(sb * EZ, 2, SUB, LANES)
    u4 = u.reshape(sb * EZ, 2, SUB, LANES)
    mz = m[:, 2].reshape(sb * EZ, 2, SUB, LANES)
    for i in range(sb * EZ):
        gz = apply_z([u4[i, 0], u4[i, 1]], consts, 0)
        out = apply_z([gz[0] * mz[i, 0], gz[1] * mz[i, 1]], consts, 16)
        for t in range(2):
            put_w(i // EZ, 2 * (i % EZ) + t, out[t] + consts[32 + t] * r[i, t])


def join_work(sb, get_w, get_flag, put_v, put_faces):
    sub, lane = iotas()
    ey, b = sub % EY, lane // 8 % 8
    up = (b == 7) & (ey < EY - 1)
    meets = up | ((b == 0) & (ey > 0))
    swap = jnp.where(b == 7, lane - 56, jnp.where(b == 0, lane + 56, lane))
    top_mask = (sub >= 4) & (lane >= 64)
    bot_mask = (sub < 4) & (lane < 64)
    group = lane // 16 % 4
    low_half = lane < 64
    pick = (lane % 16) * 8 + 7 * (lane // 64)
    every = range(sb)
    w = [[get_w(s, k) for k in range(8)] for s in every]
    crossed = [[lane_gather(w[s][k], swap) for k in range(8)] for s in every]
    v = [
        [
            w[s][k] + jnp.where(meets, jnp.where(up, roll_sub(crossed[s][k], -1), roll_sub(crossed[s][k], 1)), 0.0)
            for k in range(8)
        ]
        for s in every
    ]
    for s in every:
        for ez in range(EZ - 1):
            below, above = v[s][2 * ez + 1], v[s][2 * ez + 2]
            mixed = roll_lane(roll_sub(jnp.where(bot_mask, above, below), 4), 64)
            v[s][2 * ez + 1] = below + jnp.where(top_mask, mixed, 0.0)
            v[s][2 * ez + 2] = above + jnp.where(bot_mask, mixed, 0.0)
    for s in every:
        for k in range(8):
            put_v(s, k, v[s][k])
    packs = []
    for s in every:
        packs.append([])
        for k in range(8):
            got = lane_gather(v[s][k], pick)
            if k % 4 == 0:
                packs[s].append(got)
            else:
                packs[s][-1] = jnp.where(group == k % 4, got, packs[s][-1])
    turned = [roll_lane(packs[s][1], 64) for s in every]
    left = [jnp.where(low_half, packs[s][0], turned[s]) for s in every]
    right = [jnp.where(low_half, turned[s], packs[s][0]) for s in every]
    flags = [get_flag(s) for s in every]
    right = [jnp.where(flags[s], flip(right[s], sub, lane), right[s]) for s in every]
    for s in every:
        put_faces(0, s, right[s])
        put_faces(1, s, left[s])
    for side, (face, low, high) in enumerate(((right, 64, 56), (left, 0, 120))):
        index = lane % 8 + jnp.where(sub < 4, low, high)
        slot = (lane // 8 + jnp.where(sub < 4, 1, 0)) % 16
        edge = lane_gather(face[0], index)
        for s in every[1:]:
            edge = jnp.where(slot == s, lane_gather(face[s], index), edge)
        put_faces(3 + side, 0, roll_sub(edge, 4))
    ends = [jnp.where(sub < 4, v[s][0], v[s][7]) for s in every]
    for s in range(0, sb, 2):
        put_faces(2, s // 2, jnp.where((sub < 4) == (lane < 64), ends[s], roll_lane(ends[s + 1], 64)))


def neighbour_places(ids_ref, sb, slabs, peers, me):
    total = slabs * peers
    sub, lane = iotas()

    def row_of(device):
        start = device * slabs
        row = jnp.broadcast_to(ids_ref[pl.ds(start // LANES, 1), :], (SUB, LANES))
        return row, lax.rem(start, LANES)

    own, at = row_of(me)
    own = lane_gather(own, lax.rem(lane, slabs) + at)
    found = []
    for step in (-1, 1):
        other, at = row_of(lax.rem(me + peers + step, peers))
        want = own + step
        want = jnp.where(want < 0, total - 1, jnp.where(want >= total, 0, want))
        hits = jnp.zeros((SUB, LANES), jnp.int32)
        for j in range(slabs // SUB):
            place = j * SUB + sub
            hits = hits + jnp.where(lane_gather(other, place + at) == want, place, 0)
        for by in (4, 2, 1):
            hits = hits + roll_sub(hits, by)
        found += [hits, lax.div(hits, sb), lax.rem(LANES + 32 * (1 - step) - 8 * lax.rem(hits, sb), LANES)]
    table = found[0]
    for row in range(1, 6):
        table = jnp.where(sub == row, found[row], table)
    return table


def kernel(
    sb, blocks, peers, u_hbm, m_hbm, fm_hbm, ids_hbm, fwd_hbm, bwd_hbm, con_hbm, out_ref,
    u_buf, m_buf, fm_buf, ids_buf, fwd_buf, bwd_buf, con_buf, w_buf, place_buf, place, *refs
):
    sending, landing, (in_sem, once_sem, send_sem, recv_sem) = refs[:5], refs[5:10], refs[10:]
    slabs = sb * blocks
    me, layer = lax.axis_index("slab"), lax.axis_index("layer")
    right, left = lax.rem(me + 1, peers), lax.rem(me + peers - 1, peers)
    targets = (
        {"slab": right, "layer": layer},
        {"slab": left, "layer": layer},
        {"slab": me, "layer": 1 - layer},
        {"slab": right, "layer": 1 - layer},
        {"slab": left, "layer": 1 - layer},
    )
    sizes = (sb, sb, sb // 2, 1, 1)
    barrier = pltpu.get_barrier_semaphore()
    for target in targets:
        pl.semaphore_signal(barrier, inc=1, device_id=target, device_id_type=pl.DeviceIdType.MESH)

    def load_of(which, at):
        hbm, buf, size = ((u_hbm, u_buf, sb * 64), (m_hbm, m_buf, sb * 192))[which]
        rows = pl.ds(pl.multiple_of(at * size, size), size)
        return pltpu.make_async_copy(hbm.at[rows], buf.at[rows], in_sem.at[which, at])

    once = [
        pltpu.make_async_copy(src, dst, once_sem.at[n])
        for n, (src, dst) in enumerate(
            (
                (ids_hbm, ids_buf),
                (fwd_hbm, fwd_buf),
                (bwd_hbm, bwd_buf),
                (con_hbm, con_buf),
                (fm_hbm.at[:, pl.ds(0, LANES)], fm_buf),
            )
        )
    ]
    for copy in once:
        copy.start()
    for at in range(min(DEPTH, blocks)):
        load_of(0, at).start()
        load_of(1, at).start()

    def copy_of(which, at):
        rows = pl.ds(at * sizes[which], sizes[which])
        return pltpu.make_async_remote_copy(
            src_ref=sending[which].at[rows],
            dst_ref=landing[which].at[rows],
            send_sem=send_sem.at[which, at],
            recv_sem=recv_sem.at[which, at],
            device_id=targets[which],
            device_id_type=pl.DeviceIdType.MESH,
        )

    once[0].wait()
    place_buf[...] = neighbour_places(ids_buf, sb, slabs, peers, me)
    for copy in once[1:]:
        copy.wait()
    place_copy = pltpu.make_async_copy(place_buf, place, once_sem.at[len(once)])
    place_copy.start()

    def step(i, carry):
        @pl.when(i < blocks)
        def _():
            load_of(0, i).wait()
            load_of(1, i).wait()

        @pl.when(i + DEPTH < blocks)
        def _():
            load_of(0, i + DEPTH).start()
            load_of(1, i + DEPTH).start()

        @pl.when(i == 2)
        def _():
            pl.semaphore_wait(barrier, 5)

        @pl.when(i >= 2)
        def _():
            for which in range(5):
                copy_of(which, i - 2).start()

        now, last = jnp.minimum(i, blocks - 1), jnp.maximum(i - 1, 0)

        def get_w(s, k):
            return w_buf[pl.ds(s * 64 + k * 8, 8), :]

        def get_flag(s):
            return jnp.full((SUB, LANES), fm_buf[last * sb + s, 0]) != 0

        def put_v(s, k, value):
            out_ref[pl.ds(pl.multiple_of(last * sb * 64 + s * 64 + k * 8, 8), 8), :] = value

        def put_faces(which, s, value):
            sending[which][last * sizes[which] + s] = value

        def put_w(s, k, value):
            w_buf[pl.ds(s * 64 + k * 8, 8), :] = value

        @pl.when(i > 0)
        def _():
            join_work(sb, get_w, get_flag, put_v, put_faces)
        local_work(
            sb,
            u_buf[pl.ds(pl.multiple_of(now * sb * 64, sb * 64), sb * 64), :],
            m_buf[pl.ds(pl.multiple_of(now * sb * 192, sb * 192), sb * 192), :],
            fwd_buf[...],
            bwd_buf[...],
            con_buf,
            put_w,
        )
        return carry

    lax.fori_loop(0, blocks + 1, step, 0)
    for which in range(5):
        copy_of(which, blocks - 1).start()
    place_copy.wait()

    def collect(at, carry):
        for which in range(5):
            copy_of(which, at).wait_recv()
        return carry

    lax.fori_loop(0, blocks, collect, 0)

    sub, lane = iotas()
    a = lane % 8
    top_mask = (sub >= 4) & (lane >= 64)
    bot_mask = (sub < 4) & (lane < 64)
    low_half = lane < 64
    on_face = (a == 0) | (a == 7)
    spread = (lane // 8 + 64 * (a == 0).astype(jnp.int32), lane // 8 + 64 * (a == 7).astype(jnp.int32))
    edge_behind = ((sub < 4) & (lane // 8 == 8)) | ((sub >= 4) & (lane // 8 == 7))
    edge_ahead = ((sub < 4) & (lane // 8 == 0)) | ((sub >= 4) & (lane // 8 == 15))

    def with_edge(face_ref, edge_ref, row, s, mask):
        edge = pltpu.roll(edge_ref[place[row + 1, s]], place[row + 2, s], axis=1)
        return face_ref[place[row, s]] + jnp.where(mask, edge, 0.0)

    def finish(g, carry):
        every = range(GROUP)
        behind, ahead = [], []
        for n in every:
            s = g * GROUP + n
            behind.append(with_edge(landing[0], landing[3], 0, s, edge_behind))
            ahead.append(with_edge(landing[1], landing[4], 3, s, edge_ahead))
        flipped = [flip(ahead[n], sub, lane) for n in every]
        packs = []
        for n in every:
            flag = jnp.full((SUB, LANES), fm_buf[g * GROUP + n, 0]) != 0
            near = jnp.where(flag, flipped[n], ahead[n])
            packs.append((jnp.where(low_half, near, behind[n]), jnp.where(low_half, behind[n], near)))
        for k in range(8):
            index = spread[k // 4] + 16 * (k % 4)
            for n in every:
                rows = pl.ds(pl.multiple_of((g * GROUP + n) * 64 + k * 8, 8), 8)
                w = out_ref[rows, :] + jnp.where(on_face, lane_gather(packs[n][k // 4], index), 0.0)
                if k == 0 or k == 7:
                    z = roll_sub(landing[2][g * (GROUP // 2) + n // 2], 4)
                    z = z if n % 2 else roll_lane(z, 64)
                    w = w + jnp.where(bot_mask if k == 0 else top_mask, z, 0.0)
                out_ref[rows, :] = w
        return carry

    lax.fori_loop(0, slabs // GROUP, finish, 0)

    def drain(at, carry):
        for which in range(5):
            copy_of(which, at).wait_send()
        return carry

    lax.fori_loop(0, blocks, drain, 0)


def body(sb, peers, nodal_field, metric, slab_ids, face_map):
    slabs = nodal_field.shape[1]
    blocks = slabs // sb
    fwd_op, bwd_op, consts = tables()
    u = nodal_field.reshape(slabs, EZ, EY, 4, LANES).transpose(0, 1, 3, 2, 4).reshape(slabs * 64, LANES)
    m = (
        metric.reshape(slabs, EZ, EY, 3, 4, LANES)
        .transpose(0, 1, 3, 4, 2, 5)
        .reshape(slabs * 192, LANES)
    )
    ids = slab_ids.reshape(-1, LANES)
    f32 = jnp.float32
    counts = (slabs, slabs, slabs // 2, blocks, blocks)
    hbm = pl.BlockSpec(memory_space=pltpu.HBM)
    out = pl.pallas_call(
        functools.partial(kernel, sb, blocks, peers),
        in_specs=[hbm] * 7,
        out_specs=pl.BlockSpec(memory_space=pltpu.VMEM),
        out_shape=pltpu.VMEM((slabs * 64, LANES), f32),
        scratch_shapes=[
            pltpu.VMEM(u.shape, f32),
            pltpu.VMEM(m.shape, f32),
            pltpu.SMEM((slabs, LANES), jnp.int32),
            pltpu.VMEM(ids.shape, jnp.int32),
            pltpu.VMEM(fwd_op.shape, jnp.bfloat16),
            pltpu.VMEM(bwd_op.shape, jnp.bfloat16),
            pltpu.VMEM(consts.shape, f32),
            pltpu.VMEM((sb * 64, LANES), f32),
            pltpu.VMEM((SUB, LANES), jnp.int32),
            pltpu.SMEM((SUB, LANES), jnp.int32),
            *[pltpu.VMEM((n, SUB, LANES), f32) for n in counts],
            *[pltpu.VMEM((n, SUB, LANES), f32) for n in counts],
            pltpu.SemaphoreType.DMA((2, blocks)),
            pltpu.SemaphoreType.DMA((6,)),
            pltpu.SemaphoreType.DMA((5, blocks)),
            pltpu.SemaphoreType.DMA((5, blocks)),
        ],
        compiler_params=pltpu.CompilerParams(
            collective_id=0, has_side_effects=True, vmem_limit_bytes=40 * 2**20
        ),
        name="apply",
    )(
        *(
            pltpu.with_memory_space_constraint(x, pltpu.HBM)
            for x in (u, m, face_map, ids, jnp.asarray(fwd_op), jnp.asarray(bwd_op), jnp.asarray(consts))
        )
    )
    out = out.reshape(slabs, EZ, 4, EY, LANES).transpose(0, 1, 3, 2, 4)
    return out.reshape(1, slabs, EZ, EY, PTS)


def solution(mesh):
    return jax.shard_map(
        functools.partial(body, SB, mesh.shape["slab"]),
        mesh=mesh,
        in_specs=(
            P("layer", "slab", None, None, None),
            P("layer", "slab", None, None, None, None),
            P(),
            P("slab", None),
        ),
        out_specs=P("layer", "slab", None, None, None),
        check_vma=False,
    )
```

```python
import functools

import jax
import jax.numpy as jnp
import numpy as np
from jax import lax
from jax.experimental import pallas as pl
from jax.experimental.pallas import tpu as pltpu
from jax.sharding import PartitionSpec as P

P_SIZE = 8
PTS = 512
EY = 4
EZ = 4
SUB = 8
LANES = 128
SB = 8
DEPTH = 3
GROUP = 64


def legendre_pair(nodes, degree):
    lower = nodes * 0.0 + 1.0
    upper = nodes.copy()
    for order in range(2, degree + 1):
        lower, upper = upper, ((2 * order - 1) * nodes * upper - (order - 1) * lower) / order
    return lower, upper


def gll_tables():
    degree = P_SIZE - 1
    nodes = -np.cos(np.pi * np.arange(P_SIZE) / degree)
    for _ in range(100):
        lower, upper = legendre_pair(nodes, degree)
        nodes = nodes - (nodes * upper - lower) / ((degree + 1) * upper)
    lower, upper = legendre_pair(nodes, degree)
    rho = 2.0 / (degree * (degree + 1) * upper * upper)
    eye = np.eye(P_SIZE)
    differ = nodes[:, None] - nodes[None, :] + eye
    der = upper[:, None] / (upper[None, :] * differ) * (1.0 - eye)
    der[0, 0] = -degree * (degree + 1) / 4.0
    der[degree, degree] = degree * (degree + 1) / 4.0
    return der, rho


def two_parts(table):
    high = np.asarray(table, np.float32).astype(jnp.bfloat16)
    low = (table - high.astype(np.float64)).astype(jnp.bfloat16)
    return high, low


def tables():
    der, rho = gll_tables()
    eye8, eye2 = np.eye(8), np.eye(2)
    plane = np.tile(np.kron(rho, rho), 2)
    fwd = np.concatenate(
        [np.kron(np.eye(16), der.T) * plane, np.kron(eye2, np.kron(der.T, eye8)) * plane], 1
    )
    high, low = two_parts(fwd)
    fwd_op = np.concatenate([high, high, low], 0)
    bwd = np.concatenate([np.kron(np.eye(16), der), np.kron(eye2, np.kron(der, eye8))], 0)
    high, low = two_parts(bwd)
    half = np.concatenate([high, low], 1)
    bwd_op = np.concatenate([half, half], 0)
    l2 = (np.arange(SUB) // EY)[:, None]
    h = (np.arange(LANES) // 64)[None, :]
    low = 2 * l2 + h
    zf = np.zeros((2, 2, 2, SUB, LANES))
    zb = np.zeros((2, 2, 2, SUB, LANES))
    for l in range(2):
        for s in range(2):
            c_in = 2 * (l2 ^ s) + (h ^ l)
            for odd in range(2):
                sign = 1 - 2 * odd
                ahead = (der[low, c_in] + sign * der[low, 7 - c_in]) / 2
                back = (der[c_in, low] - sign * der[c_in, 7 - low]) / 2
                zf[odd, l, s] = np.roll(ahead * rho[low] * plane[None, :], 64 * l, 1)
                zb[odd, l, s] = np.roll(back, 64 * l, 1)
    rc = np.stack([np.broadcast_to(rho[low], (SUB, LANES)), np.broadcast_to(rho[4 + low], (SUB, LANES))])
    consts = np.concatenate([zf.reshape(-1, SUB, LANES), zb.reshape(-1, SUB, LANES), rc], 0)
    return fwd_op, bwd_op, consts.astype(np.float32)


def roll_sub(x, by):
    return pltpu.roll(x, by % SUB, axis=x.ndim - 2)


def roll_lane(x, by):
    return pltpu.roll(x, by % LANES, axis=x.ndim - 1)


def split(x):
    high = x.astype(jnp.bfloat16)
    return high, (x - high.astype(jnp.float32)).astype(jnp.bfloat16)


def iotas():
    sub = lax.broadcasted_iota(jnp.int32, (SUB, LANES), 0)
    lane = lax.broadcasted_iota(jnp.int32, (SUB, LANES), 1)
    return sub, lane


def lane_gather(x, index):
    return jnp.take_along_axis(x, index, axis=1, mode="promise_in_bounds")


def flip_sub(y, sub):
    y = jnp.where(sub % 2 == 0, roll_sub(y, -1), roll_sub(y, 1))
    return jnp.where(sub % EY < 2, roll_sub(y, -2), roll_sub(y, 2))


def turn(x):
    return roll_sub(x, 4)


def apply_z(first, last, consts, base):
    halves = []
    for odd, x in enumerate((first + last, first - last)):
        y = roll_sub(x, 4)
        at = base + 4 * odd
        halves.append([consts[at + 2 * l] * x + consts[at + 2 * l + 1] * y for l in range(2)])
    (even_near, even_far), (odd_near, odd_far) = halves
    return even_near + odd_near, even_far + odd_far, odd_near - even_near, odd_far - even_far


def forward_work(sb, u, m, fwd, put_flux):
    rows = sb * 64
    high, low = split(u)
    g = jnp.dot(jnp.concatenate([high, low, high], 1), fwd, preferred_element_type=jnp.float32)
    m = m.reshape(sb * EZ, 3, 16, LANES)
    for n in range(2):
        part = g[:, n * LANES : (n + 1) * LANES].reshape(sb * EZ, 16, LANES)
        high, low = split((part * m[:, n]).reshape(rows, LANES))
        put_flux(n, high)
        put_flux(2 + n, low)


def backward_work(sb, flux, u, m, bwd, consts, put_w):
    r = jnp.dot(flux, bwd, preferred_element_type=jnp.float32)
    r = (r[:, :LANES] + r[:, LANES:]).reshape(sb * EZ, 2, SUB, LANES)
    u4 = u.reshape(sb * EZ, 2, SUB, LANES)
    mz = m.reshape(sb * EZ, 3, 2, SUB, LANES)[:, 2]
    for i in range(sb * EZ):
        near, far, near_t, far_t = apply_z(u4[i, 0], turn(roll_lane(u4[i, 1], 64)), consts, 0)
        first = (near + roll_lane(far, 64)) * mz[i, 0]
        last = (near_t + roll_lane(far_t, 64)) * turn(roll_lane(mz[i, 1], 64))
        near, far, near_t, far_t = apply_z(first, last, consts, 8)
        out = (near + roll_lane(far, 64), turn(roll_lane(near_t, 64) + far_t))
        for t in range(2):
            put_w(i // EZ, 2 * (i % EZ) + t, out[t] + consts[16 + t] * r[i, t])


def join_work(sb, get_w, get_flag, put_v, put_faces):
    sub, lane = iotas()
    ey, b = sub % EY, lane // 8 % 8
    up = (b == 7) & (ey < EY - 1)
    meets = up | ((b == 0) & (ey > 0))
    swap = jnp.where(b == 7, lane - 56, jnp.where(b == 0, lane + 56, lane))
    top_mask = (sub >= 4) & (lane >= 64)
    bot_mask = (sub < 4) & (lane < 64)
    group = lane // 16 % 4
    low_half = lane < 64
    pick = (lane % 16) * 8 + 7 * (lane // 64)
    every = range(sb)
    w = [[get_w(s, k) for k in range(8)] for s in every]
    crossed = [[lane_gather(w[s][k], swap) for k in range(8)] for s in every]
    v = [
        [
            w[s][k] + jnp.where(meets, jnp.where(up, roll_sub(crossed[s][k], -1), roll_sub(crossed[s][k], 1)), 0.0)
            for k in range(8)
        ]
        for s in every
    ]
    for s in every:
        for ez in range(EZ - 1):
            below, above = v[s][2 * ez + 1], v[s][2 * ez + 2]
            mixed = roll_lane(roll_sub(jnp.where(bot_mask, above, below), 4), 64)
            v[s][2 * ez + 1] = below + jnp.where(top_mask, mixed, 0.0)
            v[s][2 * ez + 2] = above + jnp.where(bot_mask, mixed, 0.0)
    for s in every:
        for k in range(8):
            put_v(s, k, v[s][k])
    packs = []
    for s in every:
        packs.append([])
        for k in range(8):
            got = lane_gather(v[s][k], pick)
            if k % 4 == 0:
                packs[s].append(got)
            else:
                packs[s][-1] = jnp.where(group == k % 4, got, packs[s][-1])
    flags = [get_flag(s) for s in every]
    turned = [roll_lane(packs[s][1], 64) for s in every]
    low_flip = [lane_gather(packs[s][1], lane ^ 71) for s in every]
    high_flip = [lane_gather(packs[s][0], lane ^ 7) for s in every]
    mixed = [jnp.where(sub < 4, packs[s][0], packs[s][1]) for s in every]
    spot = jnp.where(sub < 4, 0, 56)
    edge_left = [lane_gather(mixed[s], spot + lane % 8) for s in every]
    edge_right = [lane_gather(mixed[s], spot + 64 + lane % 8) for s in every]
    edge_flip = [lane_gather(mixed[s], spot + 71 - lane % 8) for s in every]
    slot = (lane // 8 + jnp.where(sub < 4, 1, 0)) % 16
    edges = [edge_left[0], None]
    for s in every:
        put_faces(1, s, jnp.where(low_half, packs[s][0], turned[s]))
        right = jnp.where(low_half, turned[s], packs[s][0])
        flipped = flip_sub(jnp.where(low_half, low_flip[s], high_flip[s]), sub)
        put_faces(0, s, jnp.where(flags[s], flipped, right))
        edge = jnp.where(flags[s], flip_sub(edge_flip[s], sub), edge_right[s])
        edges = [
            jnp.where(slot == s, edge_left[s], edges[0]),
            edge if s == 0 else jnp.where(slot == s, edge, edges[1]),
        ]
    put_faces(3, 0, roll_sub(edges[1], 4))
    put_faces(4, 0, roll_sub(edges[0], 4))
    ends = [jnp.where(sub < 4, v[s][0], v[s][7]) for s in every]
    for s in range(0, sb, 2):
        put_faces(2, s // 2, jnp.where((sub < 4) == (lane < 64), ends[s], roll_lane(ends[s + 1], 64)))


def neighbour_places(ids_ref, sb, slabs, peers, me):
    total = slabs * peers
    sub, lane = iotas()

    def row_of(device):
        start = device * slabs
        row = jnp.broadcast_to(ids_ref[pl.ds(start // LANES, 1), :], (SUB, LANES))
        return row, lax.rem(start, LANES)

    own, at = row_of(me)
    own = lane_gather(own, lax.rem(lane, slabs) + at)
    found = []
    for step in (-1, 1):
        other, at = row_of(lax.rem(me + peers + step, peers))
        want = own + step
        want = jnp.where(want < 0, total - 1, jnp.where(want >= total, 0, want))
        hits = jnp.zeros((SUB, LANES), jnp.int32)
        for j in range(slabs // SUB):
            place = j * SUB + sub
            hits = hits + jnp.where(lane_gather(other, place + at) == want, place, 0)
        for by in (4, 2, 1):
            hits = hits + roll_sub(hits, by)
        found += [hits, lax.div(hits, sb), lax.rem(LANES + 32 * (1 - step) - 8 * lax.rem(hits, sb), LANES)]
    table = found[0]
    for row in range(1, 6):
        table = jnp.where(sub == row, found[row], table)
    return table


def kernel(
    sb, blocks, peers, u_hbm, m_hbm, fm_hbm, ids_hbm, fwd_hbm, bwd_hbm, con_hbm, out_ref,
    u_buf, m_buf, fm_buf, ids_buf, fwd_buf, bwd_buf, con_buf, w_buf, flux_buf, place_buf, place, *refs
):
    sending, landing, (in_sem, once_sem, send_sem, recv_sem) = refs[:5], refs[5:10], refs[10:]
    slabs = sb * blocks
    me, layer = lax.axis_index("slab"), lax.axis_index("layer")
    right, left = lax.rem(me + 1, peers), lax.rem(me + peers - 1, peers)
    targets = (
        {"slab": right, "layer": layer},
        {"slab": left, "layer": layer},
        {"slab": me, "layer": 1 - layer},
        {"slab": right, "layer": 1 - layer},
        {"slab": left, "layer": 1 - layer},
    )
    sizes = (sb, sb, sb // 2, 1, 1)
    barrier = pltpu.get_barrier_semaphore()

    def load_of(which, at):
        hbm, buf, size = ((u_hbm, u_buf, sb * 64), (m_hbm, m_buf, sb * 192))[which]
        rows = pl.ds(pl.multiple_of(at * size, size), size)
        return pltpu.make_async_copy(hbm.at[rows], buf.at[rows], in_sem.at[which, at])

    once = [
        pltpu.make_async_copy(src, dst, once_sem.at[n])
        for n, (src, dst) in enumerate(
            (
                (fwd_hbm, fwd_buf),
                (bwd_hbm, bwd_buf),
                (con_hbm, con_buf),
                (fm_hbm.at[:, pl.ds(0, LANES)], fm_buf),
                (ids_hbm, ids_buf),
            )
        )
    ]
    once[0].start()
    load_of(0, 0).start()
    load_of(1, 0).start()
    for copy in once[1:]:
        copy.start()
    for at in range(1, min(DEPTH, blocks)):
        load_of(0, at).start()
        load_of(1, at).start()
    for target in targets:
        pl.semaphore_signal(barrier, inc=1, device_id=target, device_id_type=pl.DeviceIdType.MESH)

    def copy_of(which, at):
        rows = pl.ds(at * sizes[which], sizes[which])
        return pltpu.make_async_remote_copy(
            src_ref=sending[which].at[rows],
            dst_ref=landing[which].at[rows],
            send_sem=send_sem.at[which, at],
            recv_sem=recv_sem.at[which, at],
            device_id=targets[which],
            device_id_type=pl.DeviceIdType.MESH,
        )

    once[0].wait()

    def step(i, carry):
        @pl.when(i < blocks)
        def _():
            load_of(0, i).wait()
            load_of(1, i).wait()

        @pl.when(i + DEPTH < blocks)
        def _():
            load_of(0, i + DEPTH).start()
            load_of(1, i + DEPTH).start()

        @pl.when(i == 1)
        def _():
            for copy in once[1:4]:
                copy.wait()

        @pl.when(i == 2)
        def _():
            pl.semaphore_wait(barrier, 5)

        @pl.when(i >= 2)
        def _():
            for which in range(5):
                copy_of(which, i - 2).start()

        now, last = jnp.minimum(i, blocks - 1), jnp.maximum(i - 1, 0)

        def get_w(s, k):
            return w_buf[pl.ds(s * 64 + k * 8, 8), :]

        def get_flag(s):
            return jnp.full((SUB, LANES), fm_buf[last * sb + s, 0]) != 0

        def put_v(s, k, value):
            out_ref[pl.ds(pl.multiple_of(last * sb * 64 + s * 64 + k * 8, 8), 8), :] = value

        def put_faces(which, s, value):
            sending[which][last * sizes[which] + s] = value

        def put_w(s, k, value):
            w_buf[pl.ds(s * 64 + k * 8, 8), :] = value

        def fields(at):
            return (
                u_buf[pl.ds(pl.multiple_of(at * sb * 64, sb * 64), sb * 64), :],
                m_buf[pl.ds(pl.multiple_of(at * sb * 192, sb * 192), sb * 192), :],
            )

        def put_flux(n, value):
            flux_buf[n] = value

        def backward():
            flux = jnp.concatenate([flux_buf[n] for n in range(4)], 1)
            backward_work(sb, flux, *fields(last), bwd_buf[...], con_buf, put_w)

        def forward():
            forward_work(sb, *fields(now), fwd_buf[...], put_flux)

        @pl.when(i == 0)
        def _():
            forward()

        @pl.when((i > 0) & (i < blocks))
        def _():
            backward()
            forward()

        @pl.when(i == blocks)
        def _():
            backward()

        @pl.when(i >= 1)
        def _():
            join_work(sb, get_w, get_flag, put_v, put_faces)

        return carry

    lax.fori_loop(0, blocks + 1, step, 0)
    for which in range(5):
        copy_of(which, blocks - 1).start()
    once[4].wait()
    place_buf[...] = neighbour_places(ids_buf, sb, slabs, peers, me)
    place_copy = pltpu.make_async_copy(place_buf, place, once_sem.at[len(once)])
    place_copy.start()
    place_copy.wait()

    def collect(at, carry):
        for which in range(5):
            copy_of(which, at).wait_recv()
        return carry

    lax.fori_loop(0, blocks, collect, 0)

    sub, lane = iotas()
    a = lane % 8
    top_mask = (sub >= 4) & (lane >= 64)
    bot_mask = (sub < 4) & (lane < 64)
    low_half = lane < 64
    on_face = (a == 0) | (a == 7)
    spread = (lane // 8 + 64 * (a == 0).astype(jnp.int32), lane // 8 + 64 * (a == 7).astype(jnp.int32))
    edge_behind = ((sub < 4) & (lane // 8 == 8)) | ((sub >= 4) & (lane // 8 == 7))
    edge_ahead = ((sub < 4) & (lane // 8 == 0)) | ((sub >= 4) & (lane // 8 == 15))

    def with_edge(face_ref, edge_ref, row, s, mask):
        edge = pltpu.roll(edge_ref[place[row + 1, s]], place[row + 2, s], axis=1)
        return face_ref[place[row, s]] + jnp.where(mask, edge, 0.0)

    def finish(g, carry):
        every = range(GROUP)
        behind, ahead = [], []
        for n in every:
            s = g * GROUP + n
            behind.append(with_edge(landing[0], landing[3], 0, s, edge_behind))
            ahead.append(with_edge(landing[1], landing[4], 3, s, edge_ahead))
        flipped = [flip_sub(lane_gather(ahead[n], lane ^ 7), sub) for n in every]
        packs = []
        for n in every:
            flag = jnp.full((SUB, LANES), fm_buf[g * GROUP + n, 0]) != 0
            near = jnp.where(flag, flipped[n], ahead[n])
            packs.append((jnp.where(low_half, near, behind[n]), jnp.where(low_half, behind[n], near)))
        for k in range(8):
            index = spread[k // 4] + 16 * (k % 4)
            for n in every:
                rows = pl.ds(pl.multiple_of((g * GROUP + n) * 64 + k * 8, 8), 8)
                w = out_ref[rows, :] + jnp.where(on_face, lane_gather(packs[n][k // 4], index), 0.0)
                if k == 0 or k == 7:
                    z = roll_sub(landing[2][g * (GROUP // 2) + n // 2], 4)
                    z = z if n % 2 else roll_lane(z, 64)
                    w = w + jnp.where(bot_mask if k == 0 else top_mask, z, 0.0)
                out_ref[rows, :] = w
        return carry

    lax.fori_loop(0, slabs // GROUP, finish, 0)

    def drain(at, carry):
        for which in range(5):
            copy_of(which, at).wait_send()
        return carry

    lax.fori_loop(0, blocks, drain, 0)


def body(sb, peers, nodal_field, metric, slab_ids, face_map):
    slabs = nodal_field.shape[1]
    blocks = slabs // sb
    fwd_op, bwd_op, consts = tables()
    u = nodal_field.reshape(slabs, EZ, EY, 4, LANES).transpose(0, 1, 3, 2, 4).reshape(slabs * 64, LANES)
    m = (
        metric.reshape(slabs, EZ, EY, 3, 4, LANES)
        .transpose(0, 1, 3, 4, 2, 5)
        .reshape(slabs * 192, LANES)
    )
    ids = slab_ids.reshape(-1, LANES)
    f32 = jnp.float32
    counts = (slabs, slabs, slabs // 2, blocks, blocks)
    hbm = pl.BlockSpec(memory_space=pltpu.HBM)
    out = pl.pallas_call(
        functools.partial(kernel, sb, blocks, peers),
        in_specs=[hbm] * 7,
        out_specs=pl.BlockSpec(memory_space=pltpu.VMEM),
        out_shape=pltpu.VMEM((slabs * 64, LANES), f32),
        scratch_shapes=[
            pltpu.VMEM(u.shape, f32),
            pltpu.VMEM(m.shape, f32),
            pltpu.SMEM((slabs, LANES), jnp.int32),
            pltpu.VMEM(ids.shape, jnp.int32),
            pltpu.VMEM(fwd_op.shape, jnp.bfloat16),
            pltpu.VMEM(bwd_op.shape, jnp.bfloat16),
            pltpu.VMEM(consts.shape, f32),
            pltpu.VMEM((sb * 64, LANES), f32),
            pltpu.VMEM((4, sb * 64, LANES), jnp.bfloat16),
            pltpu.VMEM((SUB, LANES), jnp.int32),
            pltpu.SMEM((SUB, LANES), jnp.int32),
            *[pltpu.VMEM((n, SUB, LANES), f32) for n in counts],
            *[pltpu.VMEM((n, SUB, LANES), f32) for n in counts],
            pltpu.SemaphoreType.DMA((2, blocks)),
            pltpu.SemaphoreType.DMA((6,)),
            pltpu.SemaphoreType.DMA((5, blocks)),
            pltpu.SemaphoreType.DMA((5, blocks)),
        ],
        compiler_params=pltpu.CompilerParams(
            collective_id=0, has_side_effects=True, vmem_limit_bytes=40 * 2**20
        ),
        name="apply",
    )(
        *(
            pltpu.with_memory_space_constraint(x, pltpu.HBM)
            for x in (u, m, face_map, ids, jnp.asarray(fwd_op), jnp.asarray(bwd_op), jnp.asarray(consts))
        )
    )
    out = out.reshape(slabs, EZ, 4, EY, LANES).transpose(0, 1, 3, 2, 4)
    return out.reshape(1, slabs, EZ, EY, PTS)


def solution(mesh):
    return jax.shard_map(
        functools.partial(body, SB, mesh.shape["slab"]),
        mesh=mesh,
        in_specs=(
            P("layer", "slab", None, None, None),
            P("layer", "slab", None, None, None, None),
            P(),
            P("slab", None),
        ),
        out_specs=P("layer", "slab", None, None, None),
        check_vma=False,
    )
```

```python
import functools

import jax
import jax.numpy as jnp
import numpy as np
from jax import lax
from jax.experimental import pallas as pl
from jax.experimental.pallas import tpu as pltpu
from jax.sharding import PartitionSpec as P

P_SIZE = 8
PTS = 512
EY = 4
EZ = 4
SUB = 8
LANES = 128
SB = 8
DEPTH = 3
GROUP = 64


def legendre_pair(nodes, degree):
    lower = nodes * 0.0 + 1.0
    upper = nodes.copy()
    for order in range(2, degree + 1):
        lower, upper = upper, ((2 * order - 1) * nodes * upper - (order - 1) * lower) / order
    return lower, upper


def gll_tables():
    degree = P_SIZE - 1
    nodes = -np.cos(np.pi * np.arange(P_SIZE) / degree)
    for _ in range(100):
        lower, upper = legendre_pair(nodes, degree)
        nodes = nodes - (nodes * upper - lower) / ((degree + 1) * upper)
    lower, upper = legendre_pair(nodes, degree)
    rho = 2.0 / (degree * (degree + 1) * upper * upper)
    eye = np.eye(P_SIZE)
    differ = nodes[:, None] - nodes[None, :] + eye
    der = upper[:, None] / (upper[None, :] * differ) * (1.0 - eye)
    der[0, 0] = -degree * (degree + 1) / 4.0
    der[degree, degree] = degree * (degree + 1) / 4.0
    return der, rho


def two_parts(table):
    high = np.asarray(table, np.float32).astype(jnp.bfloat16)
    low = (table - high.astype(np.float64)).astype(jnp.bfloat16)
    return high, low


def tables():
    der, rho = gll_tables()
    eye8, eye2 = np.eye(8), np.eye(2)
    plane = np.tile(np.kron(rho, rho), 2)
    fwd = np.concatenate(
        [np.kron(np.eye(16), der.T) * plane, np.kron(eye2, np.kron(der.T, eye8)) * plane], 1
    )
    high, low = two_parts(fwd)
    fwd_op = np.concatenate([high, high, low], 0)
    bwd = np.concatenate([np.kron(np.eye(16), der), np.kron(eye2, np.kron(der, eye8))], 0)
    high, low = two_parts(bwd)
    half = np.concatenate([high, low], 1)
    bwd_op = np.concatenate([half, half], 0)
    l2 = (np.arange(SUB) // EY)[:, None]
    h = (np.arange(LANES) // 64)[None, :]
    low = 2 * l2 + h
    zf = np.zeros((2, 2, 2, SUB, LANES))
    zb = np.zeros((2, 2, 2, SUB, LANES))
    for l in range(2):
        for s in range(2):
            c_in = 2 * (l2 ^ s) + (h ^ l)
            for odd in range(2):
                sign = 1 - 2 * odd
                ahead = (der[low, c_in] + sign * der[low, 7 - c_in]) / 2
                back = (der[c_in, low] - sign * der[c_in, 7 - low]) / 2
                zf[odd, l, s] = np.roll(ahead * rho[low] * plane[None, :], 64 * l, 1)
                zb[odd, l, s] = np.roll(back, 64 * l, 1)
    rc = np.stack([np.broadcast_to(rho[low], (SUB, LANES)), np.broadcast_to(rho[4 + low], (SUB, LANES))])
    consts = np.concatenate([zf.reshape(-1, SUB, LANES), zb.reshape(-1, SUB, LANES), rc], 0)
    return fwd_op, bwd_op, consts.astype(np.float32)


def roll_sub(x, by):
    return pltpu.roll(x, by % SUB, axis=x.ndim - 2)


def roll_lane(x, by):
    return pltpu.roll(x, by % LANES, axis=x.ndim - 1)


def split(x):
    high = x.astype(jnp.bfloat16)
    return high, (x - high.astype(jnp.float32)).astype(jnp.bfloat16)


def iotas():
    sub = lax.broadcasted_iota(jnp.int32, (SUB, LANES), 0)
    lane = lax.broadcasted_iota(jnp.int32, (SUB, LANES), 1)
    return sub, lane


def lane_gather(x, index):
    return jnp.take_along_axis(x, index, axis=1, mode="promise_in_bounds")


def flip_sub(y, sub):
    y = jnp.where(sub % 2 == 0, roll_sub(y, -1), roll_sub(y, 1))
    return jnp.where(sub % EY < 2, roll_sub(y, -2), roll_sub(y, 2))


def turn(x):
    return roll_sub(x, 4)


def apply_z(first, last, consts, base):
    halves = []
    for odd, x in enumerate((first + last, first - last)):
        y = roll_sub(x, 4)
        at = base + 4 * odd
        halves.append([consts[at + 2 * l] * x + consts[at + 2 * l + 1] * y for l in range(2)])
    (even_near, even_far), (odd_near, odd_far) = halves
    return even_near + odd_near, even_far + odd_far, odd_near - even_near, odd_far - even_far


def forward_work(sb, u, m, fwd, put_flux):
    rows = sb * 64
    high, low = split(u)
    g = jnp.dot(jnp.concatenate([high, low, high], 1), fwd, preferred_element_type=jnp.float32)
    m = m.reshape(sb * EZ, 3, 16, LANES)
    for n in range(2):
        part = g[:, n * LANES : (n + 1) * LANES].reshape(sb * EZ, 16, LANES)
        high, low = split((part * m[:, n]).reshape(rows, LANES))
        put_flux(n, high)
        put_flux(2 + n, low)


def backward_work(sb, flux, u, m, bwd, consts, put_w):
    r = jnp.dot(flux, bwd, preferred_element_type=jnp.float32)
    r = (r[:, :LANES] + r[:, LANES:]).reshape(sb * EZ, 2, SUB, LANES)
    u4 = u.reshape(sb * EZ, 2, SUB, LANES)
    mz = m.reshape(sb * EZ, 3, 2, SUB, LANES)[:, 2]
    for i in range(sb * EZ):
        near, far, near_t, far_t = apply_z(u4[i, 0], turn(roll_lane(u4[i, 1], 64)), consts, 0)
        first = (near + roll_lane(far, 64)) * mz[i, 0]
        last = (near_t + roll_lane(far_t, 64)) * turn(roll_lane(mz[i, 1], 64))
        near, far, near_t, far_t = apply_z(first, last, consts, 8)
        out = (near + roll_lane(far, 64), turn(roll_lane(near_t, 64) + far_t))
        for t in range(2):
            put_w(i // EZ, 2 * (i % EZ) + t, out[t] + consts[16 + t] * r[i, t])


def join_work(sb, first, get_w, get_flag, put_v, put_faces, put_edges):
    sub, lane = iotas()
    ey, b = sub % EY, lane // 8 % 8
    up = (b == 7) & (ey < EY - 1)
    meets = up | ((b == 0) & (ey > 0))
    swap = jnp.where(b == 7, lane - 56, jnp.where(b == 0, lane + 56, lane))
    top_mask = (sub >= 4) & (lane >= 64)
    bot_mask = (sub < 4) & (lane < 64)
    group = lane // 16 % 4
    low_half = lane < 64
    pick = (lane % 16) * 8 + 7 * (lane // 64)
    every = range(sb)
    w = [[get_w(s, k) for k in range(8)] for s in every]
    crossed = [[lane_gather(w[s][k], swap) for k in range(8)] for s in every]
    v = [
        [
            w[s][k] + jnp.where(meets, jnp.where(up, roll_sub(crossed[s][k], -1), roll_sub(crossed[s][k], 1)), 0.0)
            for k in range(8)
        ]
        for s in every
    ]
    for s in every:
        for ez in range(EZ - 1):
            below, above = v[s][2 * ez + 1], v[s][2 * ez + 2]
            mixed = roll_lane(roll_sub(jnp.where(bot_mask, above, below), 4), 64)
            v[s][2 * ez + 1] = below + jnp.where(top_mask, mixed, 0.0)
            v[s][2 * ez + 2] = above + jnp.where(bot_mask, mixed, 0.0)
    for s in every:
        for k in range(8):
            put_v(s, k, v[s][k])
    packs = []
    for s in every:
        packs.append([])
        for k in range(8):
            got = lane_gather(v[s][k], pick)
            if k % 4 == 0:
                packs[s].append(got)
            else:
                packs[s][-1] = jnp.where(group == k % 4, got, packs[s][-1])
    flags = [get_flag(s) for s in every]
    turned = [roll_lane(packs[s][1], 64) for s in every]
    low_flip = [lane_gather(packs[s][1], lane ^ 71) for s in every]
    high_flip = [lane_gather(packs[s][0], lane ^ 7) for s in every]
    mixed = [jnp.where(sub < 4, packs[s][0], packs[s][1]) for s in every]
    spot = jnp.where(sub < 4, 0, 56)
    edge_left = [lane_gather(mixed[s], spot + lane % 8) for s in every]
    edge_right = [lane_gather(mixed[s], spot + 64 + lane % 8) for s in every]
    edge_flip = [lane_gather(mixed[s], spot + 71 - lane % 8) for s in every]
    slot = (lane // 8 + jnp.where(sub < 4, 1, 0)) % 16 - first
    edges = [edge_left[0], None]
    for s in every:
        put_faces(1, s, jnp.where(low_half, packs[s][0], turned[s]))
        right = jnp.where(low_half, turned[s], packs[s][0])
        flipped = flip_sub(jnp.where(low_half, low_flip[s], high_flip[s]), sub)
        put_faces(0, s, jnp.where(flags[s], flipped, right))
        edge = jnp.where(flags[s], flip_sub(edge_flip[s], sub), edge_right[s])
        edges = [
            jnp.where(slot == s, edge_left[s], edges[0]),
            edge if s == 0 else jnp.where(slot == s, edge, edges[1]),
        ]
    put_edges(roll_sub(edges[1], 4), roll_sub(edges[0], 4))
    ends = [jnp.where(sub < 4, v[s][0], v[s][7]) for s in every]
    for s in range(0, sb, 2):
        put_faces(2, s // 2, jnp.where((sub < 4) == (lane < 64), ends[s], roll_lane(ends[s + 1], 64)))


def neighbour_places(ids_ref, sb, slabs, peers, me):
    total = slabs * peers
    sub, lane = iotas()

    def row_of(device):
        start = device * slabs
        row = jnp.broadcast_to(ids_ref[pl.ds(start // LANES, 1), :], (SUB, LANES))
        return row, lax.rem(start, LANES)

    own, at = row_of(me)
    own = lane_gather(own, lax.rem(lane, slabs) + at)
    found = []
    for step in (-1, 1):
        other, at = row_of(lax.rem(me + peers + step, peers))
        want = own + step
        want = jnp.where(want < 0, total - 1, jnp.where(want >= total, 0, want))
        hits = jnp.zeros((SUB, LANES), jnp.int32)
        for j in range(slabs // SUB):
            place = j * SUB + sub
            hits = hits + jnp.where(lane_gather(other, place + at) == want, place, 0)
        for by in (4, 2, 1):
            hits = hits + roll_sub(hits, by)
        found += [hits, lax.div(hits, sb), lax.rem(LANES + 32 * (1 - step) - 8 * lax.rem(hits, sb), LANES)]
    table = found[0]
    for row in range(1, 6):
        table = jnp.where(sub == row, found[row], table)
    return table


def kernel(
    sb, blocks, peers, u_hbm, m_hbm, fm_hbm, ids_hbm, fwd_hbm, bwd_hbm, con_hbm, out_ref,
    u_buf, m_buf, fm_buf, ids_buf, fwd_buf, bwd_buf, con_buf, w_buf, flux_buf, place_buf, place, *refs
):
    sending, landing, (in_sem, once_sem, send_sem, recv_sem) = refs[:5], refs[5:10], refs[10:]
    slabs = sb * blocks
    me, layer = lax.axis_index("slab"), lax.axis_index("layer")
    right, left = lax.rem(me + 1, peers), lax.rem(me + peers - 1, peers)
    targets = (
        {"slab": right, "layer": layer},
        {"slab": left, "layer": layer},
        {"slab": me, "layer": 1 - layer},
        {"slab": right, "layer": 1 - layer},
        {"slab": left, "layer": 1 - layer},
    )
    sizes = (sb, sb, sb // 2)
    barrier = pltpu.get_barrier_semaphore()

    def load_of(which, at):
        hbm, buf, size = ((u_hbm, u_buf, sb * 64), (m_hbm, m_buf, sb * 192))[which]
        rows = pl.ds(pl.multiple_of(at * size, size), size)
        return pltpu.make_async_copy(hbm.at[rows], buf.at[rows], in_sem.at[which, at])

    once = [
        pltpu.make_async_copy(src, dst, once_sem.at[n])
        for n, (src, dst) in enumerate(
            (
                (fwd_hbm, fwd_buf),
                (bwd_hbm, bwd_buf),
                (con_hbm, con_buf),
                (fm_hbm.at[:, pl.ds(0, LANES)], fm_buf),
                (ids_hbm, ids_buf),
            )
        )
    ]
    once[0].start()
    load_of(0, 0).start()
    load_of(1, 0).start()
    for copy in once[1:]:
        copy.start()
    for at in range(1, min(DEPTH, blocks)):
        load_of(0, at).start()
        load_of(1, at).start()
    for target in targets:
        pl.semaphore_signal(barrier, inc=1, device_id=target, device_id_type=pl.DeviceIdType.MESH)

    def copies(at, count):
        moves = [(which, pl.ds(at * sizes[which], count * sizes[which]), at) for which in range(3)]
        if count == 2 or at == blocks - 1:
            pair = lax.div(at, 2)
            moves += [(which, pl.ds(pair, 1), pair) for which in (3, 4)]
        return [
            pltpu.make_async_remote_copy(
                src_ref=sending[which].at[rows],
                dst_ref=landing[which].at[rows],
                send_sem=send_sem.at[which, sem],
                recv_sem=recv_sem.at[which, sem],
                device_id=targets[which],
                device_id_type=pl.DeviceIdType.MESH,
            )
            for which, rows, sem in moves
        ]

    once[0].wait()

    def step(i, carry):
        @pl.when(i < blocks)
        def _():
            load_of(0, i).wait()
            load_of(1, i).wait()

        @pl.when(i + DEPTH < blocks)
        def _():
            load_of(0, i + DEPTH).start()
            load_of(1, i + DEPTH).start()

        @pl.when(i == 1)
        def _():
            for copy in once[1:4]:
                copy.wait()

        @pl.when(i == 2)
        def _():
            pl.semaphore_wait(barrier, 5)

        @pl.when((i > 2) & (i < blocks) & (lax.rem(i, 2) == 1))
        def _():
            for copy in copies(i - 3, 2):
                copy.start()

        @pl.when(i == blocks)
        def _():
            for copy in copies(blocks - 2, 1):
                copy.start()

        now, last = jnp.minimum(i, blocks - 1), jnp.maximum(i - 1, 0)

        def join(at, count):
            def get_w(s, k):
                row = pl.multiple_of(lax.rem(at, 2) * sb * 64 + s * 64 + k * 8, 8) if count == 1 else s * 64 + k * 8
                return w_buf[pl.ds(row, 8), :]

            def get_flag(s):
                return jnp.full((SUB, LANES), fm_buf[at * sb + s, 0]) != 0

            def put_v(s, k, value):
                out_ref[pl.ds(pl.multiple_of(at * sb * 64 + s * 64 + k * 8, 8), 8), :] = value

            def put_faces(which, s, value):
                sending[which][at * sizes[which] + s] = value

            def put_edges(*edges):
                pair = lax.div(at, 2)
                for which, edge in zip((3, 4), edges):
                    if count == 1:
                        sub, lane = iotas()
                        slot = (lane // 8 + jnp.where(sub < 4, 0, 1)) % 16
                        edge = jnp.where(slot // sb == lax.rem(at, 2), edge, sending[which][pair])
                    sending[which][pair] = edge

            first = 0 if count == 2 else sb * lax.rem(at, 2)
            join_work(count * sb, first, get_w, get_flag, put_v, put_faces, put_edges)

        def put_w(s, k, value):
            w_buf[pl.ds(pl.multiple_of(lax.rem(last, 2) * sb * 64 + s * 64 + k * 8, 8), 8), :] = value

        def fields(at):
            return (
                u_buf[pl.ds(pl.multiple_of(at * sb * 64, sb * 64), sb * 64), :],
                m_buf[pl.ds(pl.multiple_of(at * sb * 192, sb * 192), sb * 192), :],
            )

        def put_flux(n, value):
            flux_buf[n] = value

        def backward():
            flux = jnp.concatenate([flux_buf[n] for n in range(4)], 1)
            backward_work(sb, flux, *fields(last), bwd_buf[...], con_buf, put_w)

        def forward():
            forward_work(sb, *fields(now), fwd_buf[...], put_flux)

        @pl.when(i == 0)
        def _():
            forward()

        @pl.when((i > 0) & (i < blocks))
        def _():
            backward()
            forward()

        @pl.when(i == blocks)
        def _():
            backward()

        @pl.when((i > 0) & (i < blocks - 1) & (lax.rem(i, 2) == 0))
        def _():
            join(i - 2, 2)

        @pl.when(i >= blocks - 1)
        def _():
            join(i - 1, 1)

        return carry

    lax.fori_loop(0, blocks + 1, step, 0)
    for copy in copies(blocks - 1, 1):
        copy.start()
    once[4].wait()
    place_buf[...] = neighbour_places(ids_buf, 2 * sb, slabs, peers, me)
    place_copy = pltpu.make_async_copy(place_buf, place, once_sem.at[len(once)])
    place_copy.start()
    place_copy.wait()

    every_copy = [copy for at in range(0, blocks - 2, 2) for copy in copies(at, 2)]
    every_copy += copies(blocks - 2, 1) + copies(blocks - 1, 1)
    for copy in every_copy:
        copy.wait_recv()

    sub, lane = iotas()
    a = lane % 8
    top_mask = (sub >= 4) & (lane >= 64)
    bot_mask = (sub < 4) & (lane < 64)
    low_half = lane < 64
    on_face = (a == 0) | (a == 7)
    spread = (lane // 8 + 64 * (a == 0).astype(jnp.int32), lane // 8 + 64 * (a == 7).astype(jnp.int32))
    edge_behind = ((sub < 4) & (lane // 8 == 8)) | ((sub >= 4) & (lane // 8 == 7))
    edge_ahead = ((sub < 4) & (lane // 8 == 0)) | ((sub >= 4) & (lane // 8 == 15))

    def with_edge(face_ref, edge_ref, row, s, mask):
        edge = pltpu.roll(edge_ref[place[row + 1, s]], place[row + 2, s], axis=1)
        return face_ref[place[row, s]] + jnp.where(mask, edge, 0.0)

    def finish(g, carry):
        every = range(GROUP)
        behind, ahead = [], []
        for n in every:
            s = g * GROUP + n
            behind.append(with_edge(landing[0], landing[3], 0, s, edge_behind))
            ahead.append(with_edge(landing[1], landing[4], 3, s, edge_ahead))
        flipped = [flip_sub(lane_gather(ahead[n], lane ^ 7), sub) for n in every]
        packs = []
        for n in every:
            flag = jnp.full((SUB, LANES), fm_buf[g * GROUP + n, 0]) != 0
            near = jnp.where(flag, flipped[n], ahead[n])
            packs.append((jnp.where(low_half, near, behind[n]), jnp.where(low_half, behind[n], near)))
        for k in range(8):
            index = spread[k // 4] + 16 * (k % 4)
            for n in every:
                rows = pl.ds(pl.multiple_of((g * GROUP + n) * 64 + k * 8, 8), 8)
                w = out_ref[rows, :] + jnp.where(on_face, lane_gather(packs[n][k // 4], index), 0.0)
                if k == 0 or k == 7:
                    z = roll_sub(landing[2][g * (GROUP // 2) + n // 2], 4)
                    z = z if n % 2 else roll_lane(z, 64)
                    w = w + jnp.where(bot_mask if k == 0 else top_mask, z, 0.0)
                out_ref[rows, :] = w
        return carry

    lax.fori_loop(0, slabs // GROUP, finish, 0)

    for copy in every_copy:
        copy.wait_send()


def body(sb, peers, nodal_field, metric, slab_ids, face_map):
    slabs = nodal_field.shape[1]
    blocks = slabs // sb
    fwd_op, bwd_op, consts = tables()
    u = nodal_field.reshape(slabs, EZ, EY, 4, LANES).transpose(0, 1, 3, 2, 4).reshape(slabs * 64, LANES)
    m = (
        metric.reshape(slabs, EZ, EY, 3, 4, LANES)
        .transpose(0, 1, 3, 4, 2, 5)
        .reshape(slabs * 192, LANES)
    )
    ids = slab_ids.reshape(-1, LANES)
    f32 = jnp.float32
    counts = (slabs, slabs, slabs // 2, blocks // 2, blocks // 2)
    hbm = pl.BlockSpec(memory_space=pltpu.HBM)
    out = pl.pallas_call(
        functools.partial(kernel, sb, blocks, peers),
        in_specs=[hbm] * 7,
        out_specs=pl.BlockSpec(memory_space=pltpu.VMEM),
        out_shape=pltpu.VMEM((slabs * 64, LANES), f32),
        scratch_shapes=[
            pltpu.VMEM(u.shape, f32),
            pltpu.VMEM(m.shape, f32),
            pltpu.SMEM((slabs, LANES), jnp.int32),
            pltpu.VMEM(ids.shape, jnp.int32),
            pltpu.VMEM(fwd_op.shape, jnp.bfloat16),
            pltpu.VMEM(bwd_op.shape, jnp.bfloat16),
            pltpu.VMEM(consts.shape, f32),
            pltpu.VMEM((2 * sb * 64, LANES), f32),
            pltpu.VMEM((4, sb * 64, LANES), jnp.bfloat16),
            pltpu.VMEM((SUB, LANES), jnp.int32),
            pltpu.SMEM((SUB, LANES), jnp.int32),
            *[pltpu.VMEM((n, SUB, LANES), f32) for n in counts],
            *[pltpu.VMEM((n, SUB, LANES), f32) for n in counts],
            pltpu.SemaphoreType.DMA((2, blocks)),
            pltpu.SemaphoreType.DMA((6,)),
            pltpu.SemaphoreType.DMA((5, blocks)),
            pltpu.SemaphoreType.DMA((5, blocks)),
        ],
        compiler_params=pltpu.CompilerParams(
            collective_id=0, has_side_effects=True, vmem_limit_bytes=40 * 2**20
        ),
        name="apply",
    )(
        *(
            pltpu.with_memory_space_constraint(x, pltpu.HBM)
            for x in (u, m, face_map, ids, jnp.asarray(fwd_op), jnp.asarray(bwd_op), jnp.asarray(consts))
        )
    )
    out = out.reshape(slabs, EZ, 4, EY, LANES).transpose(0, 1, 3, 2, 4)
    return out.reshape(1, slabs, EZ, EY, PTS)


def solution(mesh):
    return jax.shard_map(
        functools.partial(body, SB, mesh.shape["slab"]),
        mesh=mesh,
        in_specs=(
            P("layer", "slab", None, None, None),
            P("layer", "slab", None, None, None, None),
            P(),
            P("slab", None),
        ),
        out_specs=P("layer", "slab", None, None, None),
        check_vma=False,
    )
```

```python
import functools

import jax
import jax.numpy as jnp
import numpy as np
from jax import lax
from jax.experimental import pallas as pl
from jax.experimental.pallas import tpu as pltpu
from jax.sharding import PartitionSpec as P

P_SIZE = 8
PTS = 512
EY = 4
EZ = 4
SUB = 8
LANES = 128
SB = 8
DEPTH = 3
GROUP = 64


def legendre_pair(nodes, degree):
    lower = nodes * 0.0 + 1.0
    upper = nodes.copy()
    for order in range(2, degree + 1):
        lower, upper = upper, ((2 * order - 1) * nodes * upper - (order - 1) * lower) / order
    return lower, upper


def gll_tables():
    degree = P_SIZE - 1
    nodes = -np.cos(np.pi * np.arange(P_SIZE) / degree)
    for _ in range(100):
        lower, upper = legendre_pair(nodes, degree)
        nodes = nodes - (nodes * upper - lower) / ((degree + 1) * upper)
    lower, upper = legendre_pair(nodes, degree)
    rho = 2.0 / (degree * (degree + 1) * upper * upper)
    eye = np.eye(P_SIZE)
    differ = nodes[:, None] - nodes[None, :] + eye
    der = upper[:, None] / (upper[None, :] * differ) * (1.0 - eye)
    der[0, 0] = -degree * (degree + 1) / 4.0
    der[degree, degree] = degree * (degree + 1) / 4.0
    return der, rho


def two_parts(table):
    high = np.asarray(table, np.float32).astype(jnp.bfloat16)
    low = (table - high.astype(np.float64)).astype(jnp.bfloat16)
    return high, low


def tables():
    der, rho = gll_tables()
    eye8, eye2 = np.eye(8), np.eye(2)
    plane = np.tile(np.kron(rho, rho), 2)
    fwd = np.concatenate(
        [np.kron(np.eye(16), der.T) * plane, np.kron(eye2, np.kron(der.T, eye8)) * plane], 1
    )
    high, low = two_parts(fwd)
    fwd_op = np.concatenate([high, high, low], 0)
    bwd = np.concatenate([np.kron(np.eye(16), der), np.kron(eye2, np.kron(der, eye8))], 0)
    high, low = two_parts(bwd)
    half = np.concatenate([high, low], 1)
    bwd_op = np.concatenate([half, half], 0)
    l2 = (np.arange(SUB) // EY)[:, None]
    h = (np.arange(LANES) // 64)[None, :]
    low = 2 * l2 + h
    zf = np.zeros((2, 2, 2, SUB, LANES))
    zb = np.zeros((2, 2, 2, SUB, LANES))
    for l in range(2):
        for s in range(2):
            c_in = 2 * (l2 ^ s) + (h ^ l)
            for odd in range(2):
                sign = 1 - 2 * odd
                ahead = (der[low, c_in] + sign * der[low, 7 - c_in]) / 2
                back = (der[c_in, low] - sign * der[c_in, 7 - low]) / 2
                zf[odd, l, s] = np.roll(ahead * rho[low] * plane[None, :], 64 * l, 1)
                zb[odd, l, s] = np.roll(back, 64 * l, 1)
    rc = np.stack([np.broadcast_to(rho[low], (SUB, LANES)), np.broadcast_to(rho[4 + low], (SUB, LANES))])
    consts = np.concatenate([zf.reshape(-1, SUB, LANES), zb.reshape(-1, SUB, LANES), rc], 0)
    return fwd_op, bwd_op, consts.astype(np.float32)


def roll_sub(x, by):
    return pltpu.roll(x, by % SUB, axis=x.ndim - 2)


def roll_lane(x, by):
    return pltpu.roll(x, by % LANES, axis=x.ndim - 1)


def split(x):
    high = x.astype(jnp.bfloat16)
    return high, (x - high.astype(jnp.float32)).astype(jnp.bfloat16)


def iotas():
    sub = lax.broadcasted_iota(jnp.int32, (SUB, LANES), 0)
    lane = lax.broadcasted_iota(jnp.int32, (SUB, LANES), 1)
    return sub, lane


def lane_gather(x, index):
    return jnp.take_along_axis(x, index, axis=1, mode="promise_in_bounds")


def flip_sub(y, sub):
    y = jnp.where(sub % 2 == 0, roll_sub(y, -1), roll_sub(y, 1))
    return jnp.where(sub % EY < 2, roll_sub(y, -2), roll_sub(y, 2))


def turn(x):
    return roll_sub(x, 4)


def apply_z(first, last, consts, base):
    halves = []
    for odd, x in enumerate((first + last, first - last)):
        y = roll_sub(x, 4)
        at = base + 4 * odd
        halves.append([consts[at + 2 * l] * x + consts[at + 2 * l + 1] * y for l in range(2)])
    (even_near, even_far), (odd_near, odd_far) = halves
    return even_near + odd_near, even_far + odd_far, odd_near - even_near, odd_far - even_far


def forward_work(sb, u, m, fwd, put_flux):
    rows = sb * 64
    high, low = split(u)
    g = jnp.dot(jnp.concatenate([high, low, high], 1), fwd, preferred_element_type=jnp.float32)
    m = m.reshape(sb * EZ, 3, 16, LANES)
    for n in range(2):
        part = g[:, n * LANES : (n + 1) * LANES].reshape(sb * EZ, 16, LANES)
        high, low = split((part * m[:, n]).reshape(rows, LANES))
        put_flux(n, high)
        put_flux(2 + n, low)


def backward_work(sb, flux, u, m, bwd, consts, put_w):
    r = jnp.dot(flux, bwd, preferred_element_type=jnp.float32)
    r = (r[:, :LANES] + r[:, LANES:]).reshape(sb * EZ, 2, SUB, LANES)
    u4 = u.reshape(sb * EZ, 2, SUB, LANES)
    mz = m.reshape(sb * EZ, 3, 2, SUB, LANES)[:, 2]
    for i in range(sb * EZ):
        near, far, near_t, far_t = apply_z(u4[i, 0], turn(roll_lane(u4[i, 1], 64)), consts, 0)
        first = (near + roll_lane(far, 64)) * mz[i, 0]
        last = (near_t + roll_lane(far_t, 64)) * turn(roll_lane(mz[i, 1], 64))
        near, far, near_t, far_t = apply_z(first, last, consts, 8)
        out = (near + roll_lane(far, 64), turn(roll_lane(near_t, 64) + far_t))
        for t in range(2):
            put_w(i // EZ, 2 * (i % EZ) + t, out[t] + consts[16 + t] * r[i, t])


def join_work(sb, first, get_w, get_flag, put_v, put_faces, put_edges):
    sub, lane = iotas()
    ey, b = sub % EY, lane // 8 % 8
    up = (b == 7) & (ey < EY - 1)
    meets = up | ((b == 0) & (ey > 0))
    swap = jnp.where(b == 7, lane - 56, jnp.where(b == 0, lane + 56, lane))
    top_mask = (sub >= 4) & (lane >= 64)
    bot_mask = (sub < 4) & (lane < 64)
    group = lane // 16 % 4
    low_half = lane < 64
    pick = (lane % 16) * 8 + 7 * (lane // 64)
    every = range(sb)
    w = [[get_w(s, k) for k in range(8)] for s in every]
    crossed = [[lane_gather(w[s][k], swap) for k in range(8)] for s in every]
    v = [
        [
            w[s][k] + jnp.where(meets, jnp.where(up, roll_sub(crossed[s][k], -1), roll_sub(crossed[s][k], 1)), 0.0)
            for k in range(8)
        ]
        for s in every
    ]
    for s in every:
        for ez in range(EZ - 1):
            below, above = v[s][2 * ez + 1], v[s][2 * ez + 2]
            mixed = roll_lane(roll_sub(jnp.where(bot_mask, above, below), 4), 64)
            v[s][2 * ez + 1] = below + jnp.where(top_mask, mixed, 0.0)
            v[s][2 * ez + 2] = above + jnp.where(bot_mask, mixed, 0.0)
    for s in every:
        for k in range(8):
            put_v(s, k, v[s][k])
    packs = []
    for s in every:
        packs.append([])
        for k in range(8):
            got = lane_gather(v[s][k], pick)
            if k % 4 == 0:
                packs[s].append(got)
            else:
                packs[s][-1] = jnp.where(group == k % 4, got, packs[s][-1])
    flags = [get_flag(s) for s in every]
    turned = [roll_lane(packs[s][1], 64) for s in every]
    low_flip = [lane_gather(packs[s][1], lane ^ 71) for s in every]
    high_flip = [lane_gather(packs[s][0], lane ^ 7) for s in every]
    mixed = [jnp.where(sub < 4, packs[s][0], packs[s][1]) for s in every]
    spot = jnp.where(sub < 4, 0, 56)
    edge_left = [lane_gather(mixed[s], spot + lane % 8) for s in every]
    edge_right = [lane_gather(mixed[s], spot + 64 + lane % 8) for s in every]
    edge_flip = [lane_gather(mixed[s], spot + 71 - lane % 8) for s in every]
    slot = (lane // 8 + jnp.where(sub < 4, 1, 0)) % 16 - first
    edges = [edge_left[0], None]
    for s in every:
        put_faces(1, s, jnp.where(low_half, packs[s][0], turned[s]))
        right = jnp.where(low_half, turned[s], packs[s][0])
        flipped = flip_sub(jnp.where(low_half, low_flip[s], high_flip[s]), sub)
        put_faces(0, s, jnp.where(flags[s], flipped, right))
        edge = jnp.where(flags[s], flip_sub(edge_flip[s], sub), edge_right[s])
        edges = [
            jnp.where(slot == s, edge_left[s], edges[0]),
            edge if s == 0 else jnp.where(slot == s, edge, edges[1]),
        ]
    put_edges(roll_sub(edges[1], 4), roll_sub(edges[0], 4))
    ends = [jnp.where(sub < 4, v[s][0], v[s][7]) for s in every]
    for s in range(0, sb, 2):
        put_faces(2, s // 2, jnp.where((sub < 4) == (lane < 64), ends[s], roll_lane(ends[s + 1], 64)))


def neighbour_places(ids_ref, sb, slabs, peers, me):
    total = slabs * peers
    sub, lane = iotas()

    def row_of(device):
        start = device * slabs
        row = jnp.broadcast_to(ids_ref[pl.ds(start // LANES, 1), :], (SUB, LANES))
        return row, lax.rem(start, LANES)

    own, at = row_of(me)
    own = lane_gather(own, lax.rem(lane, slabs) + at)
    found = []
    for step in (-1, 1):
        other, at = row_of(lax.rem(me + peers + step, peers))
        want = own + step
        want = jnp.where(want < 0, total - 1, jnp.where(want >= total, 0, want))
        hits = jnp.zeros((SUB, LANES), jnp.int32)
        for j in range(slabs // SUB):
            place = j * SUB + sub
            hits = hits + jnp.where(lane_gather(other, place + at) == want, place, 0)
        for by in (4, 2, 1):
            hits = hits + roll_sub(hits, by)
        found += [hits, lax.div(hits, sb), lax.rem(LANES + 32 * (1 - step) - 8 * lax.rem(hits, sb), LANES)]
    table = found[0]
    for row in range(1, 6):
        table = jnp.where(sub == row, found[row], table)
    return table


def kernel(
    sb, blocks, peers, u_hbm, m_hbm, fm_hbm, ids_hbm, ops_hbm, con_hbm, out_ref,
    u_buf, m_buf, fm_buf, ids_buf, ops_buf, con_buf, w_buf, flux_buf, both_buf, place_buf, place, *refs
):
    sending, landing, (in_sem, once_sem, send_sem, recv_sem) = refs[:5], refs[5:10], refs[10:]
    slabs = sb * blocks
    me, layer = lax.axis_index("slab"), lax.axis_index("layer")
    right, left = lax.rem(me + 1, peers), lax.rem(me + peers - 1, peers)
    targets = (
        {"slab": right, "layer": layer},
        {"slab": left, "layer": layer},
        {"slab": me, "layer": 1 - layer},
        {"slab": right, "layer": 1 - layer},
        {"slab": left, "layer": 1 - layer},
    )
    sizes = (sb, sb, sb // 2)
    barrier = pltpu.get_barrier_semaphore()

    def load_of(which, at):
        hbm, buf, size = ((u_hbm, u_buf, sb * 64), (m_hbm, m_buf, sb * 192))[which]
        rows = pl.ds(pl.multiple_of(at * size, size), size)
        return pltpu.make_async_copy(hbm.at[rows], buf.at[rows], in_sem.at[which, at])

    once = [
        pltpu.make_async_copy(src, dst, once_sem.at[n])
        for n, (src, dst) in enumerate(
            (
                (ops_hbm, ops_buf),
                (con_hbm, con_buf),
                (fm_hbm.at[:, pl.ds(0, LANES)], fm_buf),
                (ids_hbm, ids_buf),
            )
        )
    ]
    once[0].start()
    load_of(0, 0).start()
    load_of(1, 0).start()
    once[1].start()
    for at in range(1, min(DEPTH, blocks)):
        load_of(0, at).start()
        load_of(1, at).start()
    once[2].start()
    once[3].start()
    for target in targets:
        pl.semaphore_signal(barrier, inc=1, device_id=target, device_id_type=pl.DeviceIdType.MESH)

    def copies(at, count):
        moves = [(which, pl.ds(at * sizes[which], count * sizes[which]), at) for which in range(3)]
        if count == 2 or at == blocks - 1:
            pair = lax.div(at, 2)
            moves += [(which, pl.ds(pair, 1), pair) for which in (3, 4)]
        return [
            pltpu.make_async_remote_copy(
                src_ref=sending[which].at[rows],
                dst_ref=landing[which].at[rows],
                send_sem=send_sem.at[which, sem],
                recv_sem=recv_sem.at[which, sem],
                device_id=targets[which],
                device_id_type=pl.DeviceIdType.MESH,
            )
            for which, rows, sem in moves
        ]

    once[0].wait()

    def step(i, carry):
        @pl.when(i < blocks)
        def _():
            load_of(0, i).wait()
            load_of(1, i).wait()

        @pl.when(i + DEPTH < blocks)
        def _():
            load_of(0, i + DEPTH).start()
            load_of(1, i + DEPTH).start()

        @pl.when(i == 1)
        def _():
            once[1].wait()

        @pl.when(i == 2)
        def _():
            once[2].wait()
            pl.semaphore_wait(barrier, 5)

        @pl.when((i > 2) & (i < blocks) & (lax.rem(i, 2) == 1))
        def _():
            for copy in copies(i - 3, 2):
                copy.start()

        @pl.when(i == blocks)
        def _():
            for copy in copies(blocks - 2, 1):
                copy.start()

        now, last = jnp.minimum(i, blocks - 1), jnp.maximum(i - 1, 0)

        def join(at, count):
            def get_w(s, k):
                row = pl.multiple_of(lax.rem(at, 2) * sb * 64 + s * 64 + k * 8, 8) if count == 1 else s * 64 + k * 8
                return w_buf[pl.ds(row, 8), :]

            def get_flag(s):
                return jnp.full((SUB, LANES), fm_buf[at * sb + s, 0]) != 0

            def put_v(s, k, value):
                out_ref[pl.ds(pl.multiple_of(at * sb * 64 + s * 64 + k * 8, 8), 8), :] = value

            def put_faces(which, s, value):
                sending[which][at * sizes[which] + s] = value

            def put_edges(*edges):
                pair = lax.div(at, 2)
                for which, edge in zip((3, 4), edges):
                    if count == 1:
                        sub, lane = iotas()
                        slot = (lane // 8 + jnp.where(sub < 4, 0, 1)) % 16
                        edge = jnp.where(slot // sb == lax.rem(at, 2), edge, sending[which][pair])
                    sending[which][pair] = edge

            first = 0 if count == 2 else sb * lax.rem(at, 2)
            join_work(count * sb, first, get_w, get_flag, put_v, put_faces, put_edges)

        def put_w(s, k, value):
            w_buf[pl.ds(pl.multiple_of(lax.rem(last, 2) * sb * 64 + s * 64 + k * 8, 8), 8), :] = value

        def fields(at):
            return (
                u_buf[pl.ds(pl.multiple_of(at * sb * 64, sb * 64), sb * 64), :],
                m_buf[pl.ds(pl.multiple_of(at * sb * 192, sb * 192), sb * 192), :],
            )

        def put_flux(n, value):
            flux_buf[n] = value

        def backward():
            flux = jnp.concatenate([flux_buf[n] for n in range(4)], 1)
            backward_work(sb, flux, *fields(last), ops_buf[3 * LANES :], con_buf, put_w)

        def forward():
            forward_work(sb, *fields(now), ops_buf[: 3 * LANES], put_flux)

        @pl.when(i == 0)
        def _():
            forward()

        @pl.when((i > 0) & (i < blocks))
        def _():
            backward()
            forward()

        @pl.when(i == blocks)
        def _():
            backward()

        @pl.when((i > 0) & (i < blocks - 1) & (lax.rem(i, 2) == 0))
        def _():
            join(i - 2, 2)

        @pl.when(i >= blocks - 1)
        def _():
            join(i - 1, 1)

        return carry

    lax.fori_loop(0, blocks + 1, step, 0)
    for copy in copies(blocks - 1, 1):
        copy.start()
    once[3].wait()
    place_buf[...] = neighbour_places(ids_buf, 2 * sb, slabs, peers, me)
    place_copy = pltpu.make_async_copy(place_buf, place, once_sem.at[len(once)])
    place_copy.start()

    sub, lane = iotas()
    a = lane % 8
    top_mask = (sub >= 4) & (lane >= 64)
    bot_mask = (sub < 4) & (lane < 64)
    low_half = lane < 64
    on_face = (a == 0) | (a == 7)
    spread = (lane // 8 + 64 * (a == 0).astype(jnp.int32), lane // 8 + 64 * (a == 7).astype(jnp.int32))
    edge_behind = ((sub < 4) & (lane // 8 == 8)) | ((sub >= 4) & (lane // 8 == 7))
    edge_ahead = ((sub < 4) & (lane // 8 == 0)) | ((sub >= 4) & (lane // 8 == 15))

    def with_edge(face, edge, by, mask):
        return face + jnp.where(mask, roll_lane(edge, by), 0.0)

    def prepare(pair):
        every = range(2 * sb)
        at = pair * 2 * sb
        ahead = [with_edge(landing[1][at + n], landing[4][pair], -8 * n, edge_ahead) for n in every]
        behind = [with_edge(landing[0][at + n], landing[3][pair], 64 - 8 * n, edge_behind) for n in every]
        flipped = [lane_gather(ahead[n], lane ^ 7) for n in every]
        for n in every:
            landing[0][at + n] = behind[n]
            both_buf[2 * (at + n)] = ahead[n]
            both_buf[2 * (at + n) + 1] = flip_sub(flipped[n], sub)

    def collect(pair, carry):
        for copy in copies(2 * pair, 2):
            copy.wait_recv()
        prepare(pair)
        return carry

    lax.fori_loop(0, blocks // 2 - 1, collect, 0)
    place_copy.wait()
    last_copies = copies(blocks - 2, 1) + copies(blocks - 1, 1)
    for copy in last_copies:
        copy.wait_recv()
    prepare(blocks // 2 - 1)

    def finish(g, carry):
        every = range(GROUP)
        packs = []
        for n in every:
            s = g * GROUP + n
            behind = landing[0][place[0, s]]
            ahead = both_buf[2 * place[3, s] + jnp.minimum(fm_buf[s, 0], 1)]
            packs.append((jnp.where(low_half, ahead, behind), jnp.where(low_half, behind, ahead)))
        for k in range(8):
            index = spread[k // 4] + 16 * (k % 4)
            for n in every:
                rows = pl.ds(pl.multiple_of((g * GROUP + n) * 64 + k * 8, 8), 8)
                w = out_ref[rows, :] + jnp.where(on_face, lane_gather(packs[n][k // 4], index), 0.0)
                if k == 0 or k == 7:
                    z = roll_sub(landing[2][g * (GROUP // 2) + n // 2], 4)
                    z = z if n % 2 else roll_lane(z, 64)
                    w = w + jnp.where(bot_mask if k == 0 else top_mask, z, 0.0)
                out_ref[rows, :] = w
        return carry

    lax.fori_loop(0, slabs // GROUP, finish, 0)

    def drain(pair, carry):
        for copy in copies(2 * pair, 2):
            copy.wait_send()
        return carry

    lax.fori_loop(0, blocks // 2 - 1, drain, 0)
    for copy in last_copies:
        copy.wait_send()


def body(sb, peers, nodal_field, metric, slab_ids, face_map):
    slabs = nodal_field.shape[1]
    blocks = slabs // sb
    fwd_op, bwd_op, consts = tables()
    ops = np.concatenate([fwd_op, bwd_op], 0)
    u = nodal_field.reshape(slabs, EZ, EY, 4, LANES).transpose(0, 1, 3, 2, 4).reshape(slabs * 64, LANES)
    m = (
        metric.reshape(slabs, EZ, EY, 3, 4, LANES)
        .transpose(0, 1, 3, 4, 2, 5)
        .reshape(slabs * 192, LANES)
    )
    ids = slab_ids.reshape(-1, LANES)
    f32 = jnp.float32
    counts = (slabs, slabs, slabs // 2, blocks // 2, blocks // 2)
    hbm = pl.BlockSpec(memory_space=pltpu.HBM)
    out = pl.pallas_call(
        functools.partial(kernel, sb, blocks, peers),
        in_specs=[hbm] * 6,
        out_specs=pl.BlockSpec(memory_space=pltpu.VMEM),
        out_shape=pltpu.VMEM((slabs * 64, LANES), f32),
        scratch_shapes=[
            pltpu.VMEM(u.shape, f32),
            pltpu.VMEM(m.shape, f32),
            pltpu.SMEM((slabs, LANES), jnp.int32),
            pltpu.VMEM(ids.shape, jnp.int32),
            pltpu.VMEM(ops.shape, jnp.bfloat16),
            pltpu.VMEM(consts.shape, f32),
            pltpu.VMEM((2 * sb * 64, LANES), f32),
            pltpu.VMEM((4, sb * 64, LANES), jnp.bfloat16),
            pltpu.VMEM((2 * slabs, SUB, LANES), f32),
            pltpu.VMEM((SUB, LANES), jnp.int32),
            pltpu.SMEM((SUB, LANES), jnp.int32),
            *[pltpu.VMEM((n, SUB, LANES), f32) for n in counts],
            *[pltpu.VMEM((n, SUB, LANES), f32) for n in counts],
            pltpu.SemaphoreType.DMA((2, blocks)),
            pltpu.SemaphoreType.DMA((6,)),
            pltpu.SemaphoreType.DMA((5, blocks)),
            pltpu.SemaphoreType.DMA((5, blocks)),
        ],
        compiler_params=pltpu.CompilerParams(
            collective_id=0, has_side_effects=True, vmem_limit_bytes=40 * 2**20
        ),
        name="apply",
    )(
        *(
            pltpu.with_memory_space_constraint(x, pltpu.HBM)
            for x in (u, m, face_map, ids, jnp.asarray(ops), jnp.asarray(consts))
        )
    )
    out = out.reshape(slabs, EZ, 4, EY, LANES).transpose(0, 1, 3, 2, 4)
    return out.reshape(1, slabs, EZ, EY, PTS)


def solution(mesh):
    return jax.shard_map(
        functools.partial(body, SB, mesh.shape["slab"]),
        mesh=mesh,
        in_specs=(
            P("layer", "slab", None, None, None),
            P("layer", "slab", None, None, None, None),
            P(),
            P("slab", None),
        ),
        out_specs=P("layer", "slab", None, None, None),
        check_vma=False,
    )
```
